32 devices in a mesh: section: 8 (over y, x, core), tensor: 4 (over z).
Axes of the slice: x: 2, y: 2, z: 4, core: 2. Of those that a mesh axis runs over, the one named last changes fastest.
Arguments:
- section_inputs: bfloat16 [8, 512, 1024], P('section', 'tensor'), may hold values from -6 to 6
- w_in: bfloat16 [8, 2304, 1024], P('section', 'tensor'), may hold values from -0.1875 to 0.1875
- in_bias: bfloat16 [8, 2304], P('section', 'tensor'), may hold values from -3 to 3
- w_out: bfloat16 [8, 2304, 1024], P('section', 'tensor'), may hold values from -0.125 to 0.125
- out_bias: float32 [8, 1024], P('section'), may hold values from -2 to 2
- norm_gain: float32 [8, 1024], P('section'), may hold values from 0.1 to 1.9
- norm_bias: float32 [8, 1024], P('section'), may hold values from -2 to 2
- patches: bfloat16 [8, 512, 1024], P(None, 'tensor'), may hold values from -6 to 6
- plan: int32 [3], replicated, may hold values from 0 to 7, as said below
Outputs:
- received: bfloat16 [8, 4, 512, 1024], P('section', None, 'tensor')
The draws below stay inside these ranges and needn't reach their ends.
Inputs may be any that keep to these rules, and one draw needn't show every extreme that they name: `plan`: the first min(8, 3) entries are all different.
All inputs are finite; a program needn't handle non-finite values.
Results may differ from the reference program's by a relative error of at most 0.0065.
Values may be sent and summed in bfloat16 or wider, within the bound.
A program may use at most 64 MiB of HBM per device.

```python
import jax
import jax.numpy as jnp
from jax import lax

D = 1024
FF = 2304
TICKS = 4
MICRO = 8
TOKG = 512
N_SECTION = 8


def draw_plan(key, part):
    order = jax.random.permutation(key, MICRO).astype(jnp.int32)
    places = jnp.arange(TICKS - 1, dtype=jnp.int32) % MICRO
    return order[places].astype(jnp.int32)


def block_scale(key, shape, shards, least, largest):
    def one(position, parts):
        heights = jax.random.uniform(jax.random.fold_in(jax.random.fold_in(key, 6), position), (parts,), jnp.float32, least / len(shards), largest / len(shards))
        return jnp.repeat(jnp.exp(heights), shape[position] // parts).reshape((-1,) + (1,) * (len(shape) - position - 1))

    level = one(*shards[0])
    for cut in shards[1:]:
        level = level * one(*cut)
    return level


def noise(own_key, shape, scale, reach, shards=(), held_as=jnp.bfloat16):
    factor_of = block_scale(own_key, shape, shards, -0.22, 0.18) if shards else 1.0
    array = jax.random.normal(own_key, shape, jnp.float32) * scale * factor_of
    return jnp.minimum(jnp.maximum(array, -reach), reach).astype(held_as)


def setup_inputs(seed: int = 0) -> dict:
    key_of = jax.random.split(jax.random.key(seed), 10)
    section_inputs = noise(key_of[0], (N_SECTION, TOKG, D), 1.0, 6.0, ((0, 8), (1, 4)))
    w_in = noise(key_of[1], (N_SECTION, FF, D), D ** -0.5, 0.1875, ((0, 8), (1, 4)))
    in_bias = noise(key_of[2], (N_SECTION, FF), 0.5, 3.0, ((0, 8), (1, 4)))
    w_out = noise(key_of[3], (N_SECTION, FF, D), FF ** -0.5, 0.125, ((0, 8), (1, 4)))
    out_bias = noise(key_of[4], (N_SECTION, D), 0.3, 2.0, ((0, 8),), jnp.float32)
    norm_gain = jnp.clip(1.0 + 0.18 * jax.random.normal(key_of[5], (N_SECTION, D), jnp.float32), 0.1, 1.9)
    norm_bias = noise(key_of[6], (N_SECTION, D), 0.3, 2.0, ((0, 8),), jnp.float32)
    patches = noise(key_of[7], (MICRO, TOKG, D), 1.0, 6.0, ((1, 4),))
    plan = draw_plan(jax.random.fold_in(key_of[9], 71), 0)
    return {"section_inputs": section_inputs, "w_in": w_in, "in_bias": in_bias, "w_out": w_out, "out_bias": out_bias, "norm_gain": norm_gain, "norm_bias": norm_bias, "patches": patches, "plan": plan}


norm_floor = 0.1
gelu_slope = 1.702

def normalize(current, gain_row, shift_row):
    widened = current.astype(jnp.float32)
    average = lax.optimization_barrier(jnp.mean(widened, axis=-1, keepdims=True))
    centered = widened - average
    variance = lax.optimization_barrier(jnp.mean(centered * centered, axis=-1, keepdims=True))
    normed = (centered * lax.rsqrt(variance + norm_floor) * gain_row + shift_row).astype(jnp.bfloat16)
    return (normed, widened)

def activate(preact):
    return preact * jax.nn.sigmoid(gelu_slope * preact)

def apply_block(current, gain_row, shift_row, full_in, full_bias, full_out, bias_row):
    normed, widened = normalize(current, gain_row, shift_row)
    preact = lax.dot_general(normed, full_in, (((1,), (1,)), ((), ())), preferred_element_type=jnp.float32)
    preact = preact + full_bias.astype(jnp.float32)
    hidden = activate(preact).astype(jnp.bfloat16)
    return (widened + jnp.dot(hidden, full_out, preferred_element_type=jnp.float32) + bias_row).astype(jnp.bfloat16)

def reference(section_inputs, w_in, in_bias, w_out, out_bias, norm_gain, norm_bias, patches, plan):
    current = section_inputs
    records = []
    for tick_index in range(TICKS):
        produced = lax.map(lambda operands: apply_block(*operands), (current, norm_gain, norm_bias, w_in, in_bias, w_out, out_bias))
        arrived = jnp.roll(produced, 1, axis=0)
        records.append(arrived)
        if tick_index + 1 < TICKS:
            selected = lax.dynamic_index_in_dim(patches, plan[tick_index], 0, keepdims=False)
            current = arrived.at[0].set(selected)
    return jnp.stack(records, axis=1)
```

```python
import functools

import jax
import jax.numpy as jnp
from jax import lax
from jax.experimental import pallas as pl
from jax.experimental.pallas import tpu as pltpu
from jax.sharding import PartitionSpec as P

TICKS = 4
CHUNKS = 4
VMEM_BYTES = 60 * 1024 * 1024

norm_floor = 0.1
gelu_slope = 1.702
MESH = pl.DeviceIdType.MESH


def activate(preact):
    return preact * jax.nn.sigmoid(gelu_slope * preact)


def normalize(widened, gain_row, shift_row):
    average = jnp.mean(widened, axis=-1, keepdims=True)
    centered = widened - average
    variance = jnp.mean(centered * centered, axis=-1, keepdims=True)
    return (centered * lax.rsqrt(variance + norm_floor) * gain_row + shift_row).astype(
        jnp.bfloat16
    )


def relay_kernel(
    n, sections, chunks,
    x_ref, win_ref, ib_ref, wout_ref, ob_ref, gain_ref, shift_ref, patches_ref, plan_ref,
    o_ref,
    gathered, part, right_out, right_in, left_out, left_in, own, produced, arrived,
    ag_send, ag_recv, rs_send, rs_recv, hop_send, hop_recv,
):
    items = TICKS * chunks
    rows, width = x_ref.shape[1], x_ref.shape[2]
    me = lax.axis_index("tensor")
    section = lax.axis_index("section")
    following = lax.rem(section + 1, sections)
    preceding = lax.rem(section + sections - 1, sections)
    has_left, has_right = me > 0, me < n - 1

    barrier = pltpu.get_barrier_semaphore()

    def greet(tensor, sect):
        pl.semaphore_signal(
            barrier, inc=1, device_id={"section": sect, "tensor": tensor}, device_id_type=MESH
        )

    greet(me, following)
    greet(me, preceding)
    pl.when(has_left)(lambda: greet(me - 1, section))
    pl.when(has_right)(lambda: greet(me + 1, section))
    pl.semaphore_wait(barrier, 2 + has_left.astype(jnp.int32) + has_right.astype(jnp.int32))

    def gather_copy(item, shard, way):
        return pltpu.make_async_remote_copy(
            src_ref=gathered.at[item, shard],
            dst_ref=gathered.at[item, shard],
            send_sem=ag_send.at[way, item, shard],
            recv_sem=ag_recv.at[way, item, shard],
            device_id={"section": section, "tensor": me + 1 if way == 0 else me - 1},
            device_id_type=MESH,
        )

    def reduce_copy(item, dest, way):
        return pltpu.make_async_remote_copy(
            src_ref=(right_out if way == 0 else left_out).at[item, dest],
            dst_ref=(right_in if way == 0 else left_in).at[item, dest],
            send_sem=rs_send.at[way, item, dest],
            recv_sem=rs_recv.at[way, item, dest],
            device_id={"section": section, "tensor": me + 1 if way == 0 else me - 1},
            device_id_type=MESH,
        )

    def relay_copy(item):
        return pltpu.make_async_remote_copy(
            src_ref=produced.at[item],
            dst_ref=arrived.at[item],
            send_sem=hop_send.at[item],
            recv_sem=hop_recv.at[item],
            device_id={"section": following, "tensor": me},
            device_id_type=MESH,
        )

    def begin(item):
        @pl.when(item < chunks)
        def _():
            own[item] = x_ref[item]

        @pl.when(item >= chunks)
        def _():
            before = item - chunks
            relay_copy(before).wait_recv()
            value = arrived[before]
            o_ref[before] = value
            own[item] = value

            @pl.when(section == 0)
            def _():
                entry = plan_ref[lax.div(before, chunks)]
                own[item] = patches_ref[entry, lax.rem(before, chunks)]

        gathered[item, me] = normalize(
            own[item].astype(jnp.float32), gain_ref[...], shift_ref[...]
        )
        pl.when(has_right)(lambda: gather_copy(item, me, 0).start())
        pl.when(has_left)(lambda: gather_copy(item, me, 1).start())

    def pass_on(item, hop):
        @pl.when(me >= hop)
        def _():
            gather_copy(item, me - hop, 0).wait_recv()
            pl.when(has_right)(lambda: gather_copy(item, me - hop, 0).start())

        @pl.when(me + hop < n)
        def _():
            gather_copy(item, me + hop, 1).wait_recv()
            pl.when(has_left)(lambda: gather_copy(item, me + hop, 1).start())

    def multiply(item):
        slot = lax.rem(item, 4)
        tokens = gathered[item].reshape(n * rows, width)
        preact = lax.dot_general(
            tokens, win_ref[...], (((1,), (1,)), ((), ())), preferred_element_type=jnp.float32
        )
        hidden = activate(preact + ib_ref[...].astype(jnp.float32)).astype(jnp.bfloat16)
        part[slot] = jnp.dot(
            hidden, wout_ref[...], preferred_element_type=jnp.float32
        ).reshape(n, rows, width)

    def reduce_step(item, hop):
        slot = lax.rem(item, 4)

        @pl.when(me == hop)
        def _():
            for dest in range(n - 1, hop - 1, -1):
                if hop > 0:
                    reduce_copy(item, dest, 0).wait_recv()
                    value = part[slot, dest] + right_in[item, dest].astype(jnp.float32)
                else:
                    value = part[slot, dest]
                if dest > hop:
                    right_out[item, dest] = value.astype(jnp.bfloat16)
                    reduce_copy(item, dest, 0).start()
                elif hop > 0:
                    part[slot, dest] = value

        mine = n - 1 - hop

        @pl.when(me == mine)
        def _():
            for dest in range(0, mine + 1):
                if hop > 0:
                    reduce_copy(item, dest, 1).wait_recv()
                    value = part[slot, dest] + left_in[item, dest].astype(jnp.float32)
                else:
                    value = part[slot, dest]
                if dest < mine:
                    left_out[item, dest] = value.astype(jnp.bfloat16)
                    reduce_copy(item, dest, 1).start()
                elif hop > 0:
                    part[slot, dest] = value

    def finish(item):
        slot = lax.rem(item, 4)
        produced[item] = (
            own[item].astype(jnp.float32) + part[slot, me] + ob_ref[...]
        ).astype(jnp.bfloat16)
        relay_copy(item).start()

    def stage(number, item):
        if number == 0:
            begin(item)
        elif number < n:
            pass_on(item, number)
        if number == n - 1:
            multiply(item)
        if number >= n - 1:
            reduce_step(item, number - (n - 1))
        if number == 2 * n - 2:
            finish(item)

    def turn(step, carry):
        for parity in range(2):
            for number in range(2 * n - 2, -1, -1):
                if number % 2 == parity:
                    item = step - number // 2
                    pl.when((item >= 0) & (item < items))(
                        functools.partial(stage, number, item)
                    )
        return carry

    lax.fori_loop(0, items + n - 1, turn, 0)

    def drain(item, carry):
        relay_copy(item).wait_send()

        @pl.when(item >= items - chunks)
        def _():
            relay_copy(item).wait_recv()
            o_ref[item] = arrived[item]

        for other in range(n):
            pl.when(has_right & (me >= other))(
                lambda: gather_copy(item, other, 0).wait_send()
            )
            pl.when(has_left & (me <= other))(
                lambda: gather_copy(item, other, 1).wait_send()
            )
            pl.when(me < other)(lambda: reduce_copy(item, other, 0).wait_send())
            pl.when(me > other)(lambda: reduce_copy(item, other, 1).wait_send())
        return carry

    lax.fori_loop(0, items, drain, 0)


def relay_call(n, sections, chunks, args):
    x, w_in, in_bias, w_out, out_bias, gain, shift, patches, plan = args
    tokens, width = x.shape
    rows = tokens // chunks
    items = TICKS * chunks
    micro = patches.shape[0]
    bf16 = jnp.bfloat16
    vmem = pl.BlockSpec(memory_space=pltpu.VMEM)
    every = (items, n, rows, width)
    dma = pltpu.SemaphoreType.DMA
    out = pl.pallas_call(
        functools.partial(relay_kernel, n, sections, chunks),
        out_shape=jax.ShapeDtypeStruct((items, rows, width), bf16),
        in_specs=[vmem] * 8 + [pl.BlockSpec(memory_space=pltpu.SMEM)],
        out_specs=vmem,
        scratch_shapes=[
            pltpu.VMEM(every, bf16),
            pltpu.VMEM((4, n, rows, width), jnp.float32),
            pltpu.VMEM(every, bf16),
            pltpu.VMEM(every, bf16),
            pltpu.VMEM(every, bf16),
            pltpu.VMEM(every, bf16),
            pltpu.VMEM((items, rows, width), bf16),
            pltpu.VMEM((items, rows, width), bf16),
            pltpu.VMEM((items, rows, width), bf16),
            dma((2, items, n)),
            dma((2, items, n)),
            dma((2, items, n)),
            dma((2, items, n)),
            dma((items,)),
            dma((items,)),
        ],
        compiler_params=pltpu.CompilerParams(
            collective_id=0, has_side_effects=True, vmem_limit_bytes=VMEM_BYTES
        ),
    )(
        x.reshape(chunks, rows, width),
        w_in,
        in_bias.reshape(1, -1),
        w_out,
        out_bias.reshape(1, -1),
        gain.reshape(1, -1),
        shift.reshape(1, -1),
        patches.reshape(micro, chunks, rows, width),
        plan,
    )
    return out.reshape(1, TICKS, tokens, width)


def passed_along(value, axis, steps):
    count = lax.axis_size(axis)
    pairs = [(source, (source + steps) % count) for source in range(count)]
    return lax.ppermute(value, axis, pairs)


def gathered_weights(args):
    current, w_in, in_bias, w_out, bias_row, gain_row, shift_row, patches, plan = args
    section_index = lax.axis_index("section")
    full_in, full_bias, full_out = (
        lax.all_gather(value, "tensor", axis=0, tiled=True) for value in (w_in, in_bias, w_out)
    )
    records = []
    for tick_index in range(TICKS):
        widened = current.astype(jnp.float32)
        normed = normalize(widened, gain_row, shift_row)
        preact = lax.dot_general(
            normed, full_in, (((1,), (1,)), ((), ())), preferred_element_type=jnp.float32
        )
        hidden = activate(preact + full_bias.astype(jnp.float32)).astype(jnp.bfloat16)
        produced = (
            widened + jnp.dot(hidden, full_out, preferred_element_type=jnp.float32) + bias_row
        ).astype(jnp.bfloat16)
        arrived = passed_along(produced, "section", 1)
        records.append(arrived)
        if tick_index + 1 < TICKS:
            selected = lax.dynamic_index_in_dim(patches, plan[tick_index], 0, keepdims=False)
            current = jnp.where(section_index == 0, selected, arrived)
    return jnp.stack(records, axis=0)[None]


def shards(n, sections, *blocks):
    args = tuple(block[0] for block in blocks[:7]) + blocks[7:]
    tokens, width = args[0].shape
    held = 2 * width * (
        TICKS * tokens * (5 * n + 4) + 2 * args[1].shape[0] + tokens * (1 + args[7].shape[0])
    ) + 16 * n * tokens * width // CHUNKS
    if tokens % (CHUNKS * 16) or n < 2 or sections < 2 or held > VMEM_BYTES * 3 // 4:
        return gathered_weights(args)
    return relay_call(n, sections, CHUNKS, args)


def solution(mesh):
    placed = (
        P("section", "tensor", None),
        P("section", "tensor", None),
        P("section", "tensor"),
        P("section", "tensor", None),
        P("section", None),
        P("section", None),
        P("section", None),
        P(None, "tensor", None),
        P(),
    )
    return jax.shard_map(
        functools.partial(shards, mesh.shape["tensor"], mesh.shape["section"]),
        mesh=mesh,
        in_specs=placed,
        out_specs=P("section", None, "tensor", None),
        check_vma=False,
    )
```

```python
import functools

import jax
import jax.numpy as jnp
from jax import lax
from jax.experimental import pallas as pl
from jax.experimental.pallas import tpu as pltpu
from jax.sharding import PartitionSpec as P

TICKS = 4
HOP_SLOTS = 2
VMEM_BYTES = 60 * 1024 * 1024

norm_floor = 0.1
gelu_slope = 1.702
MESH = pl.DeviceIdType.MESH


def activate(preact):
    return preact * jax.nn.sigmoid(gelu_slope * preact)


def normalize(widened, gain_row, shift_row):
    average = jnp.mean(widened, axis=-1, keepdims=True)
    centered = widened - average
    variance = jnp.mean(centered * centered, axis=-1, keepdims=True)
    return (centered * lax.rsqrt(variance + norm_floor) * gain_row + shift_row).astype(
        jnp.bfloat16
    )


def relay_kernel(
    n, sections, hop_slots,
    x_ref, win_ref, ib_ref, wout_ref, ob_ref, gain_ref, shift_ref, patches_ref, plan_ref,
    o_ref,
    held, sums_in, sums_out, staged, total,
    x_send, x_recv, sum_send, sum_recv, ship_send, final_recv,
):
    chunks = n * hop_slots
    items = TICKS * chunks
    pieces = x_ref.shape[0]
    me = lax.axis_index("tensor")
    section = lax.axis_index("section")
    following = lax.rem(section + 1, sections)
    preceding = lax.rem(section + sections - 1, sections)

    barrier = pltpu.get_barrier_semaphore()

    def greet(sect, tensor):
        pl.semaphore_signal(
            barrier, inc=1, device_id={"section": sect, "tensor": tensor}, device_id_type=MESH
        )

    for tensor in range(n):
        greet(following, tensor)
        greet(preceding, tensor)
        pl.when(me != tensor)(functools.partial(greet, section, tensor))
    pl.semaphore_wait(barrier, 3 * n - 1)

    def x_copy(src, group, item, sect, tensor, send_sem):
        return pltpu.make_async_remote_copy(
            src_ref=src,
            dst_ref=held.at[group, item],
            send_sem=send_sem,
            recv_sem=x_recv.at[group, item],
            device_id={"section": sect, "tensor": tensor},
            device_id_type=MESH,
        )

    def forward_copy(group, item, tensor):
        return x_copy(
            held.at[group, item], group, item, section, tensor, x_send.at[group, item]
        )

    def relay_copy(group, item):
        return x_copy(
            sums_out.at[group, item], group, item + chunks, following, me,
            sum_send.at[group, item],
        )

    def sum_copy(group, item, tensor):
        return pltpu.make_async_remote_copy(
            src_ref=sums_out.at[group, item],
            dst_ref=sums_in.at[group, item],
            send_sem=sum_send.at[group, item],
            recv_sem=sum_recv.at[group, item],
            device_id={"section": section, "tensor": tensor},
            device_id_type=MESH,
        )

    def final_copy(group, item, tick, piece, home):
        return pltpu.make_async_remote_copy(
            src_ref=sums_out.at[group, item],
            dst_ref=o_ref.at[tick, piece],
            send_sem=sum_send.at[group, item],
            recv_sem=final_recv.at[tick, piece],
            device_id={"section": following, "tensor": home},
            device_id_type=MESH,
        )

    def place(group, item):
        tick, chunk = lax.div(item, chunks), lax.rem(item, chunks)
        shard, piece = lax.div(chunk, pieces), lax.rem(chunk, pieces)
        home = jnp.where(group == 0, shard, n - 1 - shard)
        right = lax.rem(jnp.minimum(tick, section) + group, 2) == 0
        position = jnp.where(right, me, n - 1 - me)
        target = jnp.where(right, me + 1, me - 1)
        return tick, piece, home, position, target

    my_group = jnp.where(me < n // 2, 0, 1)
    my_start = my_group * (n - 1)
    my_first = jnp.where(me < n // 2, me, n - 1 - me) * pieces

    def enter(tick, piece, carry):
        item = tick * chunks + my_first + piece
        if tick == 0:
            source = x_ref.at[piece]
        else:
            source = staged.at[tick - 1, piece]
            staged[tick - 1, piece] = patches_ref[plan_ref[tick - 1], piece]

        @pl.when(me == my_start)
        def _():
            held[my_group, item] = source[...]

        @pl.when(me != my_start)
        def _():
            x_copy(
                source, my_group, item, section, my_start, ship_send.at[tick, piece]
            ).start()

        return carry

    lax.fori_loop(0, pieces, functools.partial(enter, 0), 0)

    @pl.when(section == 0)
    def _():
        for tick in range(1, TICKS):
            lax.fori_loop(0, pieces, functools.partial(enter, tick), 0)

    def receive(group, item, position):
        tick, piece, home, where, target = place(group, item)

        @pl.when(where == position)
        def _():
            entered = (position == 0) & (home == me) & ((tick == 0) | (section == 0))

            @pl.when(jnp.logical_not(entered))
            def _():
                forward_copy(group, item, target).wait_recv()

            @pl.when(position < n - 1)
            def _():
                forward_copy(group, item, target).start()

            @pl.when((tick > 0) & (section > 0) & (home == me))
            def _():
                o_ref[tick - 1, piece] = held[group, item]

    def compute(group, item, position):
        tick, piece, home, where, target = place(group, item)

        @pl.when(where == position)
        def _():
            normed = normalize(
                held[group, item].astype(jnp.float32), gain_ref[...], shift_ref[...]
            )
            preact = lax.dot_general(
                normed, win_ref[...], (((1,), (1,)), ((), ())),
                preferred_element_type=jnp.float32,
            )
            hidden = activate(preact + ib_ref[...].astype(jnp.float32)).astype(jnp.bfloat16)
            total[...] = jnp.dot(hidden, wout_ref[...], preferred_element_type=jnp.float32)

            @pl.when(position > 0)
            def _():
                sum_copy(group, item, target).wait_recv()
                total[...] += sums_in[group, item].astype(jnp.float32)

            @pl.when(position < n - 1)
            def _():
                sums_out[group, item] = total[...].astype(jnp.bfloat16)
                sum_copy(group, item, target).start()

            @pl.when(position == n - 1)
            def _():
                sums_out[group, item] = (
                    held[group, item].astype(jnp.float32) + total[...] + ob_ref[...]
                ).astype(jnp.bfloat16)
                leaves = (tick == TICKS - 1) | (following == 0)

                @pl.when(leaves)
                def _():
                    final_copy(group, item, tick, piece, home).start()

                @pl.when(jnp.logical_not(leaves))
                def _():
                    relay_copy(group, item).start()

    def each(action, slot):
        def one(index, carry):
            group, position = lax.rem(index, 2), n - 1 - lax.div(index, 2)
            item = slot - position * hop_slots
            pl.when((item >= 0) & (item < items))(
                functools.partial(action, group, item, position)
            )
            return carry

        lax.fori_loop(0, 2 * n, one, 0)

    def turn(slot, carry):
        each(receive, slot)
        each(compute, slot)
        return carry

    lax.fori_loop(0, items + (n - 1) * hop_slots, turn, 0)

    def drain(item, carry):
        for group in range(2):
            tick, piece, home, position, target = place(group, item)

            @pl.when(position < n - 1)
            def _():
                forward_copy(group, item, target).wait_send()

            sum_copy(group, item, target).wait_send()

            @pl.when((home == me) & ((tick == TICKS - 1) | (section == 0)))
            def _():
                final_copy(group, item, tick, piece, home).wait_recv()

            sent = (home == me) & (me != my_start) & ((tick == 0) | (section == 0))

            @pl.when(sent)
            def _():
                x_copy(
                    staged.at[0, piece], group, item, section, my_start,
                    ship_send.at[tick, piece],
                ).wait_send()

        return carry

    lax.fori_loop(0, items, drain, 0)


def relay_call(n, sections, hop_slots, args):
    x, w_in, in_bias, w_out, out_bias, gain, shift, patches, plan = args
    tokens, width = x.shape
    pieces = 2 * hop_slots
    rows = tokens // pieces
    items = TICKS * n * hop_slots
    micro = patches.shape[0]
    bf16 = jnp.bfloat16
    vmem = pl.BlockSpec(memory_space=pltpu.VMEM)
    every = (2, items, rows, width)
    dma = pltpu.SemaphoreType.DMA
    out = pl.pallas_call(
        functools.partial(relay_kernel, n, sections, hop_slots),
        out_shape=jax.ShapeDtypeStruct((TICKS, pieces, rows, width), bf16),
        in_specs=[vmem] * 8 + [pl.BlockSpec(memory_space=pltpu.SMEM)],
        out_specs=vmem,
        scratch_shapes=[
            pltpu.VMEM(every, bf16),
            pltpu.VMEM(every, bf16),
            pltpu.VMEM(every, bf16),
            pltpu.VMEM((TICKS - 1, pieces, rows, width), bf16),
            pltpu.VMEM((rows, width), jnp.float32),
            dma((2, items)),
            dma((2, items)),
            dma((2, items)),
            dma((2, items)),
            dma((TICKS, pieces)),
            dma((TICKS, pieces)),
        ],
        compiler_params=pltpu.CompilerParams(
            collective_id=0, has_side_effects=True, vmem_limit_bytes=VMEM_BYTES
        ),
    )(
        x.reshape(pieces, rows, width),
        w_in,
        in_bias.reshape(1, -1),
        w_out,
        out_bias.reshape(1, -1),
        gain.reshape(1, -1),
        shift.reshape(1, -1),
        patches.reshape(micro, pieces, rows, width),
        plan,
    )
    return out.reshape(1, TICKS, tokens, width)


def passed_along(value, axis, steps):
    count = lax.axis_size(axis)
    pairs = [(source, (source + steps) % count) for source in range(count)]
    return lax.ppermute(value, axis, pairs)


def gathered_weights(args):
    current, w_in, in_bias, w_out, bias_row, gain_row, shift_row, patches, plan = args
    section_index = lax.axis_index("section")
    full_in, full_bias, full_out = (
        lax.all_gather(value, "tensor", axis=0, tiled=True) for value in (w_in, in_bias, w_out)
    )
    records = []
    for tick_index in range(TICKS):
        widened = current.astype(jnp.float32)
        normed = normalize(widened, gain_row, shift_row)
        preact = lax.dot_general(
            normed, full_in, (((1,), (1,)), ((), ())), preferred_element_type=jnp.float32
        )
        hidden = activate(preact + full_bias.astype(jnp.float32)).astype(jnp.bfloat16)
        produced = (
            widened + jnp.dot(hidden, full_out, preferred_element_type=jnp.float32) + bias_row
        ).astype(jnp.bfloat16)
        arrived = passed_along(produced, "section", 1)
        records.append(arrived)
        if tick_index + 1 < TICKS:
            selected = lax.dynamic_index_in_dim(patches, plan[tick_index], 0, keepdims=False)
            current = jnp.where(section_index == 0, selected, arrived)
    return jnp.stack(records, axis=0)[None]


def shards(n, sections, *blocks):
    args = tuple(block[0] for block in blocks[:7]) + blocks[7:]
    tokens, width = args[0].shape
    room = 2 * width * (
        tokens * (TICKS * (3 * n + 2) + 1 + args[7].shape[0]) + 2 * args[1].shape[0]
    )
    if tokens % (HOP_SLOTS * 32) or n % 2 or sections < 2 or room > VMEM_BYTES * 3 // 4:
        return gathered_weights(args)
    return relay_call(n, sections, HOP_SLOTS, args)


def solution(mesh):
    placed = (
        P("section", "tensor", None),
        P("section", "tensor", None),
        P("section", "tensor"),
        P("section", "tensor", None),
        P("section", None),
        P("section", None),
        P("section", None),
        P(None, "tensor", None),
        P(),
    )
    return jax.shard_map(
        functools.partial(shards, mesh.shape["tensor"], mesh.shape["section"]),
        mesh=mesh,
        in_specs=placed,
        out_specs=P("section", None, "tensor", None),
        check_vma=False,
    )
```

```python
import functools

import jax
import jax.numpy as jnp
from jax import lax
from jax.experimental import pallas as pl
from jax.experimental.pallas import tpu as pltpu
from jax.sharding import PartitionSpec as P

TICKS = 4
PIECES = 4
HOP_SLOTS = 2
VMEM_BYTES = 60 * 1024 * 1024

norm_floor = 0.1
gelu_slope = 1.702
MESH = pl.DeviceIdType.MESH


def activate(preact):
    return preact * jax.nn.sigmoid(gelu_slope * preact)


def normalize(widened, gain_row, shift_row):
    average = jnp.mean(widened, axis=-1, keepdims=True)
    centered = widened - average
    variance = jnp.mean(centered * centered, axis=-1, keepdims=True)
    return (centered * lax.rsqrt(variance + norm_floor) * gain_row + shift_row).astype(
        jnp.bfloat16
    )


def relay_kernel(
    n, sections, hop_slots,
    x_ref, win_hbm, ib_ref, wout_hbm, ob_ref, gain_ref, shift_ref, patches_hbm, plan_ref,
    o_ref,
    win_ref, wout_ref, patches_ref, load_sem, held, sums_in, sums_out, staged, total,
    x_send, x_recv, sum_send, sum_recv, ship_send, final_recv,
):
    pieces = x_ref.shape[0]
    chunks = n // 2 * pieces
    items = TICKS * chunks
    me = lax.axis_index("tensor")
    section = lax.axis_index("section")
    following = lax.rem(section + 1, sections)
    preceding = lax.rem(section + sections - 1, sections)

    loads = [
        pltpu.make_async_copy(source, target, load_sem.at[index])
        for index, (source, target) in enumerate(
            [(win_hbm, win_ref), (wout_hbm, wout_ref), (patches_hbm, patches_ref)]
        )
    ]
    for load in loads[:2]:
        load.start()
    pl.when(section == 0)(loads[2].start)

    barrier = pltpu.get_barrier_semaphore()

    def greet(sect, tensor):
        pl.semaphore_signal(
            barrier, inc=1, device_id={"section": sect, "tensor": tensor}, device_id_type=MESH
        )

    for tensor in range(n):
        greet(following, tensor)
        greet(preceding, tensor)
        pl.when(me != tensor)(functools.partial(greet, section, tensor))
    pl.semaphore_wait(barrier, 3 * n - 1)

    def x_copy(src, group, item, sect, tensor, send_sem):
        return pltpu.make_async_remote_copy(
            src_ref=src,
            dst_ref=held.at[group, item],
            send_sem=send_sem,
            recv_sem=x_recv.at[group, item],
            device_id={"section": sect, "tensor": tensor},
            device_id_type=MESH,
        )

    def forward_copy(group, item, tensor):
        return x_copy(
            held.at[group, item], group, item, section, tensor, x_send.at[group, item]
        )

    def relay_copy(group, item):
        return x_copy(
            sums_out.at[group, item], group, item + chunks, following, me,
            sum_send.at[group, item],
        )

    def sum_copy(group, item, tensor):
        return pltpu.make_async_remote_copy(
            src_ref=sums_out.at[group, item],
            dst_ref=sums_in.at[group, item],
            send_sem=sum_send.at[group, item],
            recv_sem=sum_recv.at[group, item],
            device_id={"section": section, "tensor": tensor},
            device_id_type=MESH,
        )

    def final_copy(group, item, tick, piece, home):
        return pltpu.make_async_remote_copy(
            src_ref=sums_out.at[group, item],
            dst_ref=o_ref.at[tick, piece],
            send_sem=sum_send.at[group, item],
            recv_sem=final_recv.at[tick, piece],
            device_id={"section": following, "tensor": home},
            device_id_type=MESH,
        )

    def entry_side(origin):
        later = sections - 1 - origin
        far = (origin >= 0) & (later < TICKS) & (lax.rem(later, 2) == 0)
        return far.astype(jnp.int32)

    def place(group, item):
        tick, chunk = lax.div(item, chunks), lax.rem(item, chunks)
        shard, piece = lax.div(chunk, pieces), lax.rem(chunk, pieces)
        home = jnp.where(group == 0, shard, n - 1 - shard)
        turns = jnp.minimum(tick, section) + entry_side(section - tick) + group
        right = lax.rem(turns, 2) == 0
        position = jnp.where(right, me, n - 1 - me)
        target = jnp.where(right, me + 1, me - 1)
        return tick, piece, home, position, target

    my_group = jnp.where(me < n // 2, 0, 1)
    my_start = lax.rem(my_group + entry_side(section), 2) * (n - 1)
    my_side = my_group * (n - 1)
    my_first = jnp.where(me < n // 2, me, n - 1 - me) * pieces

    def enter(tick, piece, carry):
        item = tick * chunks + my_first + piece
        if tick == 0:
            source, start = x_ref.at[piece], my_start
        else:
            start = my_side
            source = staged.at[tick - 1, piece]
            staged[tick - 1, piece] = patches_ref[plan_ref[tick - 1], piece]

        held[my_group, item] = source[...]

        @pl.when(me != start)
        def _():
            x_copy(
                source, my_group, item, section, start, ship_send.at[tick, piece]
            ).start()

        return carry

    lax.fori_loop(0, pieces, functools.partial(enter, 0), 0)

    @pl.when(section == 0)
    def _():
        loads[2].wait()
        for tick in range(1, TICKS):
            lax.fori_loop(0, pieces, functools.partial(enter, tick), 0)

    for load in loads[:2]:
        load.wait()

    def receive(group, item, position):
        tick, piece, home, where, target = place(group, item)

        @pl.when(where == position)
        def _():
            entry = (tick == 0) | (section == 0)

            @pl.when(jnp.logical_not(entry & (home == me)))
            def _():
                forward_copy(group, item, target).wait_recv()

            @pl.when((position < n - 1) & jnp.logical_not(entry & (home == target)))
            def _():
                forward_copy(group, item, target).start()

            @pl.when((tick > 0) & (section > 0) & (home == me))
            def _():
                o_ref[tick - 1, piece] = held[group, item]

    def compute(group, item, position):
        tick, piece, home, where, target = place(group, item)

        @pl.when(where == position)
        def _():
            normed = normalize(
                held[group, item].astype(jnp.float32), gain_ref[...], shift_ref[...]
            )
            preact = lax.dot_general(
                normed, win_ref[...], (((1,), (1,)), ((), ())),
                preferred_element_type=jnp.float32,
            )
            hidden = activate(preact + ib_ref[...].astype(jnp.float32)).astype(jnp.bfloat16)
            total[...] = jnp.dot(hidden, wout_ref[...], preferred_element_type=jnp.float32)

            @pl.when(position > 0)
            def _():
                sum_copy(group, item, target).wait_recv()
                total[...] += sums_in[group, item].astype(jnp.float32)

            @pl.when(position < n - 1)
            def _():
                sums_out[group, item] = total[...].astype(jnp.bfloat16)
                sum_copy(group, item, target).start()

            @pl.when(position == n - 1)
            def _():
                sums_out[group, item] = (
                    held[group, item].astype(jnp.float32) + total[...] + ob_ref[...]
                ).astype(jnp.bfloat16)
                leaves = (tick == TICKS - 1) | (following == 0)

                @pl.when(leaves)
                def _():
                    final_copy(group, item, tick, piece, home).start()

                @pl.when(jnp.logical_not(leaves))
                def _():
                    relay_copy(group, item).start()

    def each(action, slot):
        def one(index, carry):
            group, position = lax.rem(index, 2), n - 1 - lax.div(index, 2)
            item = slot - position * hop_slots
            pl.when((item >= 0) & (item < items))(
                functools.partial(action, group, item, position)
            )
            return carry

        lax.fori_loop(0, 2 * n, one, 0)

    def turn(slot, carry):
        each(receive, slot)
        each(compute, slot)
        return carry

    lax.fori_loop(0, items + (n - 1) * hop_slots, turn, 0)

    def drain(item, carry):
        for group in range(2):
            tick, piece, home, position, target = place(group, item)

            entry = (tick == 0) | (section == 0)

            @pl.when((position < n - 1) & jnp.logical_not(entry & (home == target)))
            def _():
                forward_copy(group, item, target).wait_send()

            sum_copy(group, item, target).wait_send()

            @pl.when((home == me) & ((tick == TICKS - 1) | (section == 0)))
            def _():
                final_copy(group, item, tick, piece, home).wait_recv()

            start = jnp.where(tick == 0, my_start, my_side)
            sent = (home == me) & (me != start) & entry

            @pl.when(sent)
            def _():
                x_copy(
                    staged.at[0, piece], group, item, section, start,
                    ship_send.at[tick, piece],
                ).wait_send()

        return carry

    lax.fori_loop(0, items, drain, 0)


def relay_call(n, sections, pieces, hop_slots, args):
    x, w_in, in_bias, w_out, out_bias, gain, shift, patches, plan = args
    tokens, width = x.shape
    rows = tokens // pieces
    items = TICKS * n // 2 * pieces
    micro = patches.shape[0]
    bf16 = jnp.bfloat16
    vmem = pl.BlockSpec(memory_space=pltpu.VMEM)
    hbm = pl.BlockSpec(memory_space=pl.ANY)
    every = (2, items, rows, width)
    dma = pltpu.SemaphoreType.DMA
    out = pl.pallas_call(
        functools.partial(relay_kernel, n, sections, hop_slots),
        out_shape=jax.ShapeDtypeStruct((TICKS, pieces, rows, width), bf16),
        in_specs=[vmem, hbm, vmem, hbm, vmem, vmem, vmem, hbm]
        + [pl.BlockSpec(memory_space=pltpu.SMEM)],
        out_specs=vmem,
        scratch_shapes=[
            pltpu.VMEM(w_in.shape, bf16),
            pltpu.VMEM(w_out.shape, bf16),
            pltpu.VMEM((micro, pieces, rows, width), bf16),
            dma((3,)),
            pltpu.VMEM(every, bf16),
            pltpu.VMEM(every, bf16),
            pltpu.VMEM(every, bf16),
            pltpu.VMEM((TICKS - 1, pieces, rows, width), bf16),
            pltpu.VMEM((rows, width), jnp.float32),
            dma((2, items)),
            dma((2, items)),
            dma((2, items)),
            dma((2, items)),
            dma((TICKS, pieces)),
            dma((TICKS, pieces)),
        ],
        compiler_params=pltpu.CompilerParams(
            collective_id=0, has_side_effects=True, vmem_limit_bytes=VMEM_BYTES
        ),
    )(
        x.reshape(pieces, rows, width),
        w_in,
        in_bias.reshape(1, -1),
        w_out,
        out_bias.reshape(1, -1),
        gain.reshape(1, -1),
        shift.reshape(1, -1),
        patches.reshape(micro, pieces, rows, width),
        plan,
    )
    return out.reshape(1, TICKS, tokens, width)


def passed_along(value, axis, steps):
    count = lax.axis_size(axis)
    pairs = [(source, (source + steps) % count) for source in range(count)]
    return lax.ppermute(value, axis, pairs)


def gathered_weights(args):
    current, w_in, in_bias, w_out, bias_row, gain_row, shift_row, patches, plan = args
    section_index = lax.axis_index("section")
    full_in, full_bias, full_out = (
        lax.all_gather(value, "tensor", axis=0, tiled=True) for value in (w_in, in_bias, w_out)
    )
    records = []
    for tick_index in range(TICKS):
        widened = current.astype(jnp.float32)
        normed = normalize(widened, gain_row, shift_row)
        preact = lax.dot_general(
            normed, full_in, (((1,), (1,)), ((), ())), preferred_element_type=jnp.float32
        )
        hidden = activate(preact + full_bias.astype(jnp.float32)).astype(jnp.bfloat16)
        produced = (
            widened + jnp.dot(hidden, full_out, preferred_element_type=jnp.float32) + bias_row
        ).astype(jnp.bfloat16)
        arrived = passed_along(produced, "section", 1)
        records.append(arrived)
        if tick_index + 1 < TICKS:
            selected = lax.dynamic_index_in_dim(patches, plan[tick_index], 0, keepdims=False)
            current = jnp.where(section_index == 0, selected, arrived)
    return jnp.stack(records, axis=0)[None]


def shards(n, sections, *blocks):
    args = tuple(block[0] for block in blocks[:7]) + blocks[7:]
    tokens, width = args[0].shape
    room = 2 * width * (
        tokens * (TICKS * (3 * n + 2) + 1 + args[7].shape[0]) + 2 * args[1].shape[0]
    )
    if tokens % (PIECES * 16) or n % 2 or sections < 2 or room > VMEM_BYTES * 3 // 4:
        return gathered_weights(args)
    return relay_call(n, sections, PIECES, HOP_SLOTS, args)


def solution(mesh):
    placed = (
        P("section", "tensor", None),
        P("section", "tensor", None),
        P("section", "tensor"),
        P("section", "tensor", None),
        P("section", None),
        P("section", None),
        P("section", None),
        P(None, "tensor", None),
        P(),
    )
    return jax.shard_map(
        functools.partial(shards, mesh.shape["tensor"], mesh.shape["section"]),
        mesh=mesh,
        in_specs=placed,
        out_specs=P("section", None, "tensor", None),
        check_vma=False,
    )
```

```python
import functools

import jax
import jax.numpy as jnp
from jax import lax
from jax.experimental import pallas as pl
from jax.experimental.pallas import tpu as pltpu
from jax.sharding import PartitionSpec as P

TICKS = 4
PIECES = 4
HOP_SLOTS = 2
VMEM_BYTES = 60 * 1024 * 1024

norm_floor = 0.1
gelu_slope = 1.702
MESH = pl.DeviceIdType.MESH


def activate(preact):
    return preact * jax.nn.sigmoid(gelu_slope * preact)


def normalize(widened, gain_row, shift_row):
    average = jnp.mean(widened, axis=-1, keepdims=True)
    centered = widened - average
    variance = jnp.mean(centered * centered, axis=-1, keepdims=True)
    return (centered * lax.rsqrt(variance + norm_floor) * gain_row + shift_row).astype(
        jnp.bfloat16
    )


def relay_kernel(
    n, sections, hop_slots,
    x_ref, win_hbm, ib_ref, wout_hbm, ob_ref, gain_ref, shift_ref, patches_hbm, plan_ref,
    o_ref,
    win_ref, wout_ref, patches_ref, load_sem, held, sums_in, sums_out, staged, total,
    x_send, x_recv, sum_send, sum_recv, ship_send, final_recv,
):
    pieces = x_ref.shape[0]
    chunks = n // 2 * pieces
    items = TICKS * chunks
    me = lax.axis_index("tensor")
    section = lax.axis_index("section")
    following = lax.rem(section + 1, sections)
    preceding = lax.rem(section + sections - 1, sections)

    loads = [
        pltpu.make_async_copy(source, target, load_sem.at[index])
        for index, (source, target) in enumerate(
            [(win_hbm, win_ref), (wout_hbm, wout_ref), (patches_hbm, patches_ref)]
        )
    ]
    for load in loads[:2]:
        load.start()
    pl.when(section == 0)(loads[2].start)

    barrier = pltpu.get_barrier_semaphore()

    def greet(sect, tensor):
        pl.semaphore_signal(
            barrier, inc=1, device_id={"section": sect, "tensor": tensor}, device_id_type=MESH
        )

    for tensor in range(n):
        greet(following, tensor)
        greet(preceding, tensor)
        pl.when(me != tensor)(functools.partial(greet, section, tensor))
    pl.semaphore_wait(barrier, 3 * n - 1)

    def x_copy(src, group, item, sect, tensor, send_sem):
        return pltpu.make_async_remote_copy(
            src_ref=src,
            dst_ref=held.at[group, item],
            send_sem=send_sem,
            recv_sem=x_recv.at[group, item],
            device_id={"section": sect, "tensor": tensor},
            device_id_type=MESH,
        )

    def forward_copy(group, item, tensor):
        return x_copy(
            held.at[group, item], group, item, section, tensor, x_send.at[group, item]
        )

    def relay_copy(group, item):
        return x_copy(
            sums_out.at[group, item], group, item + chunks, following, me,
            sum_send.at[group, item],
        )

    def sum_copy(group, item, tensor):
        return pltpu.make_async_remote_copy(
            src_ref=sums_out.at[group, item],
            dst_ref=sums_in.at[group, item],
            send_sem=sum_send.at[group, item],
            recv_sem=sum_recv.at[group, item],
            device_id={"section": section, "tensor": tensor},
            device_id_type=MESH,
        )

    def final_copy(group, item, tick, piece, home):
        return pltpu.make_async_remote_copy(
            src_ref=sums_out.at[group, item],
            dst_ref=o_ref.at[tick, piece],
            send_sem=sum_send.at[group, item],
            recv_sem=final_recv.at[tick, piece],
            device_id={"section": following, "tensor": home},
            device_id_type=MESH,
        )

    def entry_side(origin):
        later = sections - 1 - origin
        far = (origin >= 0) & (later < TICKS) & (lax.rem(later, 2) == 0)
        return far.astype(jnp.int32)

    def place(group, item):
        tick, chunk = lax.div(item, chunks), lax.rem(item, chunks)
        shard, piece = lax.div(chunk, pieces), lax.rem(chunk, pieces)
        home = jnp.where(group == 0, shard, n - 1 - shard)
        turns = jnp.minimum(tick, section) + entry_side(section - tick) + group
        right = lax.rem(turns, 2) == 0
        position = jnp.where(right, me, n - 1 - me)
        target = jnp.where(right, me + 1, me - 1)
        return tick, piece, home, position, target

    my_group = jnp.where(me < n // 2, 0, 1)
    my_start = lax.rem(my_group + entry_side(section), 2) * (n - 1)
    my_side = my_group * (n - 1)
    my_first = jnp.where(me < n // 2, me, n - 1 - me) * pieces

    def enter(tick, piece, carry):
        item = tick * chunks + my_first + piece
        if tick == 0:
            source, start = x_ref.at[piece], my_start
        else:
            start = my_side
            source = staged.at[tick - 1, piece]
            staged[tick - 1, piece] = patches_ref[plan_ref[tick - 1], piece]

        held[my_group, item] = source[...]

        @pl.when(me != start)
        def _():
            x_copy(
                source, my_group, item, section, start, ship_send.at[tick, piece]
            ).start()

        return carry

    lax.fori_loop(0, pieces, functools.partial(enter, 0), 0)

    @pl.when(section == 0)
    def _():
        loads[2].wait()
        for tick in range(1, TICKS):
            lax.fori_loop(0, pieces, functools.partial(enter, tick), 0)

    def receive(group, item, position):
        tick, piece, home, where, target = place(group, item)

        @pl.when(where == position)
        def _():
            entry = (tick == 0) | (section == 0)

            @pl.when(jnp.logical_not(entry & (home == me)))
            def _():
                forward_copy(group, item, target).wait_recv()

            @pl.when((position < n - 1) & jnp.logical_not(entry & (home == target)))
            def _():
                forward_copy(group, item, target).start()

            @pl.when((tick > 0) & (section > 0) & (home == me))
            def _():
                o_ref[tick - 1, piece] = held[group, item]

    def compute(group, item, position):
        tick, piece, home, where, target = place(group, item)

        @pl.when(where == position)
        def _():
            normed = normalize(
                held[group, item].astype(jnp.float32), gain_ref[...], shift_ref[...]
            )
            preact = lax.dot_general(
                normed, win_ref[...], (((1,), (1,)), ((), ())),
                preferred_element_type=jnp.float32,
            )
            hidden = activate(preact + ib_ref[...].astype(jnp.float32)).astype(jnp.bfloat16)
            total[...] = jnp.dot(hidden, wout_ref[...], preferred_element_type=jnp.float32)

            @pl.when(position > 0)
            def _():
                sum_copy(group, item, target).wait_recv()
                total[...] += sums_in[group, item].astype(jnp.float32)

            @pl.when(position < n - 1)
            def _():
                sums_out[group, item] = total[...].astype(jnp.bfloat16)
                sum_copy(group, item, target).start()

            @pl.when(position == n - 1)
            def _():
                sums_out[group, item] = (
                    held[group, item].astype(jnp.float32) + total[...] + ob_ref[...]
                ).astype(jnp.bfloat16)
                leaves = (tick == TICKS - 1) | (following == 0)

                @pl.when(leaves)
                def _():
                    final_copy(group, item, tick, piece, home).start()

                @pl.when(jnp.logical_not(leaves))
                def _():
                    relay_copy(group, item).start()

    def each(action, slot):
        def one(index, carry):
            group, position = lax.rem(index, 2), lax.div(index, 2)
            item = slot - position * hop_slots
            pl.when((item >= 0) & (item < items))(
                functools.partial(action, group, item, position)
            )
            return carry

        lax.fori_loop(0, 2 * n, one, 0)

    def turn(slot, carry):
        each(compute, slot)
        each(receive, slot + 1)
        return carry

    each(receive, 0)
    for load in loads[:2]:
        load.wait()
    lax.fori_loop(0, items + (n - 1) * hop_slots, turn, 0)

    def drain(item, carry):
        for group in range(2):
            tick, piece, home, position, target = place(group, item)

            entry = (tick == 0) | (section == 0)

            @pl.when((position < n - 1) & jnp.logical_not(entry & (home == target)))
            def _():
                forward_copy(group, item, target).wait_send()

            sum_copy(group, item, target).wait_send()

            @pl.when((home == me) & ((tick == TICKS - 1) | (section == 0)))
            def _():
                final_copy(group, item, tick, piece, home).wait_recv()

            start = jnp.where(tick == 0, my_start, my_side)
            sent = (home == me) & (me != start) & entry

            @pl.when(sent)
            def _():
                x_copy(
                    staged.at[0, piece], group, item, section, start,
                    ship_send.at[tick, piece],
                ).wait_send()

        return carry

    lax.fori_loop(0, items, drain, 0)


def relay_call(n, sections, pieces, hop_slots, args):
    x, w_in, in_bias, w_out, out_bias, gain, shift, patches, plan = args
    tokens, width = x.shape
    rows = tokens // pieces
    items = TICKS * n // 2 * pieces
    micro = patches.shape[0]
    bf16 = jnp.bfloat16
    vmem = pl.BlockSpec(memory_space=pltpu.VMEM)
    hbm = pl.BlockSpec(memory_space=pl.ANY)
    every = (2, items, rows, width)
    dma = pltpu.SemaphoreType.DMA
    out = pl.pallas_call(
        functools.partial(relay_kernel, n, sections, hop_slots),
        out_shape=jax.ShapeDtypeStruct((TICKS, pieces, rows, width), bf16),
        in_specs=[vmem, hbm, vmem, hbm, vmem, vmem, vmem, hbm]
        + [pl.BlockSpec(memory_space=pltpu.SMEM)],
        out_specs=vmem,
        scratch_shapes=[
            pltpu.VMEM(w_in.shape, bf16),
            pltpu.VMEM(w_out.shape, bf16),
            pltpu.VMEM((micro, pieces, rows, width), bf16),
            dma((3,)),
            pltpu.VMEM(every, bf16),
            pltpu.VMEM(every, bf16),
            pltpu.VMEM(every, bf16),
            pltpu.VMEM((TICKS - 1, pieces, rows, width), bf16),
            pltpu.VMEM((rows, width), jnp.float32),
            dma((2, items)),
            dma((2, items)),
            dma((2, items)),
            dma((2, items)),
            dma((TICKS, pieces)),
            dma((TICKS, pieces)),
        ],
        compiler_params=pltpu.CompilerParams(
            collective_id=0, has_side_effects=True, vmem_limit_bytes=VMEM_BYTES
        ),
    )(
        x.reshape(pieces, rows, width),
        w_in,
        in_bias.reshape(1, -1),
        w_out,
        out_bias.reshape(1, -1),
        gain.reshape(1, -1),
        shift.reshape(1, -1),
        patches.reshape(micro, pieces, rows, width),
        plan,
    )
    return out.reshape(1, TICKS, tokens, width)


def passed_along(value, axis, steps):
    count = lax.axis_size(axis)
    pairs = [(source, (source + steps) % count) for source in range(count)]
    return lax.ppermute(value, axis, pairs)


def gathered_weights(args):
    current, w_in, in_bias, w_out, bias_row, gain_row, shift_row, patches, plan = args
    section_index = lax.axis_index("section")
    full_in, full_bias, full_out = (
        lax.all_gather(value, "tensor", axis=0, tiled=True) for value in (w_in, in_bias, w_out)
    )
    records = []
    for tick_index in range(TICKS):
        widened = current.astype(jnp.float32)
        normed = normalize(widened, gain_row, shift_row)
        preact = lax.dot_general(
            normed, full_in, (((1,), (1,)), ((), ())), preferred_element_type=jnp.float32
        )
        hidden = activate(preact + full_bias.astype(jnp.float32)).astype(jnp.bfloat16)
        produced = (
            widened + jnp.dot(hidden, full_out, preferred_element_type=jnp.float32) + bias_row
        ).astype(jnp.bfloat16)
        arrived = passed_along(produced, "section", 1)
        records.append(arrived)
        if tick_index + 1 < TICKS:
            selected = lax.dynamic_index_in_dim(patches, plan[tick_index], 0, keepdims=False)
            current = jnp.where(section_index == 0, selected, arrived)
    return jnp.stack(records, axis=0)[None]


def shards(n, sections, *blocks):
    args = tuple(block[0] for block in blocks[:7]) + blocks[7:]
    tokens, width = args[0].shape
    room = 2 * width * (
        tokens * (TICKS * (3 * n + 2) + 1 + args[7].shape[0]) + 2 * args[1].shape[0]
    )
    if tokens % (PIECES * 16) or n % 2 or sections < 2 or room > VMEM_BYTES * 3 // 4:
        return gathered_weights(args)
    return relay_call(n, sections, PIECES, HOP_SLOTS, args)


def solution(mesh):
    placed = (
        P("section", "tensor", None),
        P("section", "tensor", None),
        P("section", "tensor"),
        P("section", "tensor", None),
        P("section", None),
        P("section", None),
        P("section", None),
        P(None, "tensor", None),
        P(),
    )
    return jax.shard_map(
        functools.partial(shards, mesh.shape["tensor"], mesh.shape["section"]),
        mesh=mesh,
        in_specs=placed,
        out_specs=P("section", None, "tensor", None),
        check_vma=False,
    )
```
